32 devices in a mesh: dp: 8 (over y, x, core), mp: 4 (over z).
Axes of the slice: x: 2, y: 2, z: 4, core: 2. Of those that a mesh axis runs over, the one named last changes fastest.
Arguments:
- patches: bfloat16 [192, 64, 1024], P(('dp', 'mp')), may hold values from -6 to 6
- gain_first: float32 [1024], replicated, may hold values from 0.1 to 1.9
- joint_weight: bfloat16 [1024, 3, 1024], P('dp', None, 'mp'), may hold values from -0.1875 to 0.1875
- head_scale: float32 [16], P('mp'), may hold values from 2 to 32
- output_weight: bfloat16 [1024, 1024], P('mp', 'dp'), may hold values from -0.1875 to 0.1875
- gain_second: float32 [1024], replicated, may hold values from 0.3 to 3
- up_weight: bfloat16 [1024, 4096], P('dp', 'mp'), may hold values from -0.1875 to 0.1875
- down_weight: bfloat16 [4096, 1024], P('mp', 'dp'), may hold values from -0.09375 to 0.09375
- gain_final: float32 [1024], replicated, may hold values from 0.1 to 1.9
- project_weight: bfloat16 [1024, 768], replicated, may hold values from -0.1875 to 0.1875
- text_bank: bfloat16 [3072, 768], P(('dp', 'mp')), may hold values from -20000 to 20000
- captions: int32 [192], replicated, may hold values from 0 to 3071
- reference_loss: float32 [192], P(('dp', 'mp')), may hold values from 2 to 20
Outputs:
- learnability: float32 [192], P(('dp', 'mp'))
The draws below stay inside these ranges and needn't reach their ends.
All inputs are finite; a program needn't handle non-finite values.
Results may differ from the reference program's by a relative error of at most 0.018.
Values may be sent and summed in bfloat16 or wider, within the bound.
A program may use at most 128 MiB of HBM per device.

```python
import math
import jax
import jax.numpy as jnp
from jax import lax

D = 1024
H = 16
HD = 64
FF = 4096
P_SIZE = 64
E = 768
IMG_DEV = 24
IMAGES = 192
TEXTS = 3072
N_MP = 4


def draw_text_bank(key, part):
    key_dir = jax.random.fold_in(key, 11)
    key_len = jax.random.fold_in(key, 12)
    direction = jax.random.truncated_normal(key_dir, -4.0, 4.0, (TEXTS, E), jnp.float32)
    growth = jnp.exp(math.log(3.0) * jnp.arange(TEXTS, dtype=jnp.float32)[:, None] / max(TEXTS - 1, 1))
    lengths = jnp.exp(jax.random.uniform(key_len, (TEXTS, 1), jnp.float32, math.log(12.0), math.log(120.0))) * growth
    return (direction * lengths / math.sqrt(E)).astype(jnp.bfloat16)


def place_ends(array, rng, least, largest):
    spot = [jax.random.randint(jax.random.fold_in(rng, axis), (), 0, length) for axis, length in enumerate(array.shape)]
    widest = array.shape.index(max(array.shape))
    neighbour = spot[:widest] + [(spot[widest] + 1) % array.shape[widest]] + spot[widest + 1:]
    return array.at[tuple(spot)].set(least).at[tuple(neighbour)].set(largest)


def level_of(key, extent, cuts, least, largest):
    loudness, own = 1.0, jax.random.fold_in(key, 6)
    for axis_at, shards_of in cuts:
        draws = jnp.exp(jax.random.uniform(jax.random.fold_in(own, axis_at), (shards_of,), jnp.float32, least / len(cuts), largest / len(cuts)))
        loudness = loudness * jnp.repeat(draws, extent[axis_at] // shards_of).reshape([-1 if axis == axis_at else 1 for axis in range(len(extent))])
    return loudness


def centred(stream_key, dims, width, limit, pieces=(), kind=jnp.bfloat16):
    array = jax.random.normal(stream_key, dims, jnp.float32) * width
    if len(pieces) > 0:
        array = level_of(stream_key, dims, pieces, -0.22, 0.18) * array
    return jnp.clip(array, min=-limit, max=limit).astype(kind)


def setup_inputs(seed: int = 0) -> dict:
    key_of = jax.random.split(jax.random.key(seed), 14)
    patches = centred(key_of[0], (IMAGES, P_SIZE, D), 1.0, 6.0, ((0, 32),))
    gain_first = jnp.clip(1.0 + 0.18 * jax.random.normal(key_of[1], (D,), jnp.float32), 0.1, 1.9)
    joint_weight = centred(key_of[2], (D, 3, D), D ** -0.5, 0.1875, ((0, 8), (2, 4)))
    head_scale = jnp.clip(jnp.exp(math.log(32.0) - 2.7725887 * jax.random.uniform(key_of[3], (H,), jnp.float32) ** level_of(key_of[3], (H,), ((0, 4),), -0.2, 0.2)), 2.0, 32.0)
    output_weight = centred(key_of[4], (D, D), D ** -0.5, 0.1875, ((0, 4), (1, 8)))
    gain_second = jnp.clip(jnp.exp(jax.random.uniform(key_of[5], (D,), jnp.float32, math.log(0.3), math.log(3.0))), 0.3, 3.0)
    up_weight = centred(key_of[6], (D, FF), D ** -0.5, 0.1875, ((0, 8), (1, 4)))
    down_weight = centred(key_of[7], (FF, D), FF ** -0.5, 0.09375, ((0, 4), (1, 8)))
    gain_final = jnp.clip(1.0 + 0.18 * jax.random.normal(key_of[8], (D,), jnp.float32), 0.1, 1.9)
    project_weight = centred(key_of[9], (D, E), D ** -0.5, 0.1875)
    text_bank = draw_text_bank(jax.random.fold_in(key_of[13], 71), 0)
    captions = place_ends(jax.random.randint(key_of[11], (IMAGES,), 0, TEXTS), jax.random.fold_in(key_of[11], 1), 0, TEXTS - 1).astype(jnp.int32)
    reference_loss = jnp.clip(2.0 + 18.0 * jax.random.uniform(key_of[12], (IMAGES,), jnp.float32) ** level_of(key_of[12], (IMAGES,), ((0, 32),), -0.2, 0.2), 2.0, 20.0)
    return dict(patches=patches, gain_first=gain_first, joint_weight=joint_weight, head_scale=head_scale, output_weight=output_weight, gain_second=gain_second, up_weight=up_weight, down_weight=down_weight, gain_final=gain_final, project_weight=project_weight, text_bank=text_bank, captions=captions, reference_loss=reference_loss)


def layer_norm(values, gain):
    centre = values - lax.optimization_barrier(jnp.mean(values, axis=-1, keepdims=True))
    spread = lax.optimization_barrier(jnp.mean(centre * centre, axis=-1, keepdims=True))
    return centre * lax.rsqrt(spread + 1e-06) * gain

def unit_rows(values):
    return values * lax.rsqrt(lax.optimization_barrier(jnp.sum(values * values, axis=-1, keepdims=True)) + 1e-06)

def grouped_product(left_rows, right_cols, groups):
    group_width = left_rows.shape[1] // groups
    totals = jnp.zeros((left_rows.shape[0], right_cols.shape[1]), jnp.float32)
    for index_group in range(groups):
        lower = index_group * group_width
        partial_value = jnp.dot(left_rows[:, lower:lower + group_width], right_cols[lower:lower + group_width], preferred_element_type=jnp.float32)
        rounded = lax.optimization_barrier(partial_value.astype(jnp.bfloat16))
        totals = totals + rounded.astype(jnp.float32)
    return totals

def reference(patches, gain_first, joint_weight, head_scale, output_weight, gain_second, up_weight, down_weight, gain_final, project_weight, text_bank, captions, reference_loss):

    def encode(image_block):
        amount = image_block.shape[0]
        residual = image_block.astype(jnp.float32).reshape(amount * P_SIZE, D)
        normed_first = layer_norm(residual, gain_first).astype(jnp.bfloat16)
        joint = jnp.dot(normed_first, joint_weight.reshape(D, 3 * D), preferred_element_type=jnp.float32)
        joint = joint.reshape(amount, P_SIZE, 3, H, HD)
        queries = unit_rows(joint[:, :, 0]).astype(jnp.bfloat16)
        key_rows = unit_rows(joint[:, :, 1]).astype(jnp.bfloat16)
        value_rows = joint[:, :, 2].astype(jnp.bfloat16)
        scores = jnp.einsum('bqhd,bkhd->bhqk', queries.astype(jnp.float32), key_rows.astype(jnp.float32))
        exponent = jnp.exp(scores * head_scale[None, :, None, None])
        attention = (exponent / lax.optimization_barrier(jnp.sum(exponent, axis=-1, keepdims=True))).astype(jnp.bfloat16)
        head_out = jnp.einsum('bhqk,bkhd->bqhd', attention.astype(jnp.float32), value_rows.astype(jnp.float32))
        head_out = head_out.astype(jnp.bfloat16).reshape(amount * P_SIZE, D)
        residual_two = residual + grouped_product(head_out, output_weight, N_MP)
        normed_second = layer_norm(residual_two, gain_second).astype(jnp.bfloat16)
        upper = jnp.dot(normed_second, up_weight, preferred_element_type=jnp.float32)
        hidden = jax.nn.gelu(upper, approximate=False).astype(jnp.bfloat16)
        feed = grouped_product(hidden, down_weight, N_MP)
        pooled = lax.optimization_barrier(jnp.mean((residual_two + feed).reshape(amount, P_SIZE, D), axis=1))
        pooled_norm = layer_norm(pooled, gain_final).astype(jnp.bfloat16)
        embedded = jnp.dot(pooled_norm, project_weight, preferred_element_type=jnp.float32)
        return unit_rows(embedded).astype(jnp.bfloat16)
    image_blocks = patches.reshape(IMAGES // IMG_DEV, IMG_DEV, P_SIZE, D)
    image_units = lax.map(encode, image_blocks).reshape(IMAGES, E)
    logits = jnp.dot(image_units, text_bank.T, preferred_element_type=jnp.float32)
    highest = lax.optimization_barrier(jnp.max(logits, axis=1))
    totals = lax.optimization_barrier(jnp.sum(jnp.exp(logits - highest[:, None]), axis=1))
    matched = jnp.take_along_axis(logits, captions.astype(jnp.int32)[:, None], axis=1)[:, 0]
    loss = highest + jnp.log(totals) - matched
    return loss - reference_loss
```

```python
import functools

import jax
import jax.numpy as jnp
from jax import lax
from jax.experimental import pallas as pl
from jax.experimental.pallas import tpu as pltpu
from jax.sharding import PartitionSpec as P

MESH = pl.DeviceIdType.MESH
Z, X, Y, D0, D1, S_COL, S_X, S_Y, S_D0, S_D1 = range(10)
KINDS = 10


def flip(index, bit):
    return index + bit - 2 * bit * ((index // bit) % 2)


def gather_kernel(n_mp, own_ref, full_ref, send_sem, recv_sem, local_sem):
    parts, rows, _ = own_ref.shape
    dp, mp = lax.axis_index("dp"), lax.axis_index("mp")
    sib, xn, yn = flip(dp, 1), flip(dp, 2), flip(dp, 4)
    dn = flip(xn, 4)
    right, left = lax.rem(mp + 1, n_mp), lax.rem(mp + n_mp - 1, n_mp)

    barrier = pltpu.get_barrier_semaphore()
    for target in ((dp, right), (dp, left), (xn, mp), (yn, mp), (sib, mp)):
        pl.semaphore_signal(barrier, inc=1, device_id=target, device_id_type=MESH)
    pl.semaphore_wait(barrier, 5)

    half = rows // 2

    def slot(part, step, owner, piece):
        source = lax.rem(mp - step + n_mp, n_mp)
        first = owner * rows + (half if piece == 1 else 0)
        count = rows if piece is None else half
        return full_ref.at[part, source, pl.ds(pl.multiple_of(first, half), count), :]

    def copy(kind, part, step, owner, piece, target):
        index = (part * n_mp + step) * KINDS + kind
        place = slot(part, step, owner, piece)
        src = own_ref.at[part] if step == 0 and owner is dp else place
        return pltpu.make_async_remote_copy(
            src_ref=src, dst_ref=place, send_sem=send_sem.at[index], recv_sem=recv_sem.at[index],
            device_id=target, device_id_type=MESH,
        )

    def arrival(kind, part, step, sem_step, owner, piece):
        index = (part * n_mp + sem_step) * KINDS + kind
        place = slot(part, step, owner, piece)
        pltpu.make_async_remote_copy(
            src_ref=place, dst_ref=place, send_sem=send_sem.at[index], recv_sem=recv_sem.at[index],
            device_id=(sib, mp), device_id_type=MESH,
        ).wait_recv()

    sent = []

    def send(*args):
        item = copy(*args)
        item.start()
        sent.append(item)

    steps = [(part, step) for part in range(parts) for step in range(n_mp)]
    local = []
    for part in range(parts):
        item = pltpu.make_async_copy(own_ref.at[part], slot(part, 0, dp, None), local_sem.at[part])
        item.start()
        local.append(item)

    def along_ring(at):
        if at < len(steps):
            part, step = steps[at]
            if step > 0:
                arrival(Z, part, step, step - 1, dp, None)
            if step < n_mp - 1:
                send(Z, part, step, dp, None, (dp, right))

    along_ring(0)
    for at in range(len(steps) + 2):
        along_ring(at + 1)
        if at < len(steps):
            part, step = steps[at]
            send(X, part, step, dp, None, (xn, mp))
            send(Y, part, step, dp, None, (yn, mp))
            send(S_COL, part, step, dp, None, (sib, mp))
        if 0 <= at - 1 < len(steps):
            part, step = steps[at - 1]
            arrival(X, part, step, step, xn, None)
            send(D0, part, step, xn, 0, (yn, mp))
            send(S_X, part, step, xn, None, (sib, mp))
            arrival(Y, part, step, step, yn, None)
            send(D1, part, step, yn, 1, (xn, mp))
            send(S_Y, part, step, yn, None, (sib, mp))
        if 0 <= at - 2 < len(steps):
            part, step = steps[at - 2]
            arrival(D0, part, step, step, dn, 0)
            send(S_D0, part, step, dn, 0, (sib, mp))
            arrival(D1, part, step, step, dn, 1)
            send(S_D1, part, step, dn, 1, (sib, mp))
    for part, step in steps:
        arrival(S_COL, part, step, step, flip(dp, 1), None)
        arrival(S_X, part, step, step, flip(xn, 1), None)
        arrival(S_Y, part, step, step, flip(yn, 1), None)
        arrival(S_D0, part, step, step, flip(dn, 1), 0)
        arrival(S_D1, part, step, step, flip(dn, 1), 1)
    for item in sent:
        item.wait_send()
    for item in local:
        item.wait()


def gather_weights(own, n_dp, n_mp):
    parts, rows, columns = own.shape
    if n_dp != 2 ** 3:
        full = lax.all_gather(own, "dp", axis=1, tiled=True)
        return lax.all_gather(full, "mp", axis=1)
    count = parts * n_mp * KINDS
    return pl.pallas_call(
        functools.partial(gather_kernel, n_mp),
        out_shape=jax.ShapeDtypeStruct((parts, n_mp, n_dp * rows, columns), own.dtype),
        in_specs=[pl.BlockSpec(memory_space=pltpu.VMEM)],
        out_specs=pl.BlockSpec(memory_space=pl.ANY),
        scratch_shapes=[
            pltpu.SemaphoreType.DMA((count,)),
            pltpu.SemaphoreType.DMA((count,)),
            pltpu.SemaphoreType.DMA((parts,)),
        ],
        compiler_params=pltpu.CompilerParams(collective_id=0, has_side_effects=True),
        name="gather_weights",
    )(own)


def layer_norm(values, gain):
    centre = values - jnp.mean(values, axis=-1, keepdims=True)
    spread = jnp.mean(centre * centre, axis=-1, keepdims=True)
    return centre * lax.rsqrt(spread + 1e-06) * gain


def unit_rows(values):
    return values * lax.rsqrt(jnp.sum(values * values, axis=-1, keepdims=True) + 1e-06)


def dot(left, right):
    return jnp.dot(left, right, preferred_element_type=jnp.float32)


def dot_t(left, right):
    return lax.dot_general(left, right, (((1,), (1,)), ((), ())), preferred_element_type=jnp.float32)


def grouped(values):
    return values.astype(jnp.bfloat16).astype(jnp.float32)


def shards(
    patches,
    gain_first,
    joint_weight,
    head_scale,
    output_weight,
    gain_second,
    up_weight,
    down_weight,
    gain_final,
    project_weight,
    text_bank,
    captions,
    reference_loss,
):
    n_dp, n_mp = lax.axis_size("dp"), lax.axis_size("mp")
    own_images, patch_count, features = patches.shape
    rows = joint_weight.shape[0]
    local_heads = head_scale.shape[0]
    width = joint_weight.shape[2]
    head_width = width // local_heads
    tokens = own_images * patch_count

    attention_part = jnp.concatenate([joint_weight.reshape(rows, 3 * width), output_weight.T], axis=1)
    own = jnp.stack([attention_part, up_weight, down_weight.T])
    full = gather_weights(own, n_dp, n_mp)
    scales = lax.all_gather(head_scale, "mp", axis=0, tiled=True)

    residual = patches.astype(jnp.float32).reshape(tokens, features)
    normed_first = layer_norm(residual, gain_first).astype(jnp.bfloat16)
    joint = jnp.stack([dot(normed_first, full[0, m, :, : 3 * width]) for m in range(n_mp)], axis=1)
    joint = joint.reshape(own_images, patch_count, n_mp, 3, local_heads, head_width)
    queries = unit_rows(joint[:, :, :, 0]).astype(jnp.bfloat16)
    key_rows = unit_rows(joint[:, :, :, 1]).astype(jnp.bfloat16)
    value_rows = joint[:, :, :, 2].astype(jnp.bfloat16)
    scores = jnp.einsum("bqmhd,bkmhd->bmhqk", queries, key_rows, preferred_element_type=jnp.float32)
    exponent = jnp.exp(scores * scales.reshape(n_mp, local_heads)[None, :, :, None, None])
    attention = (exponent / jnp.sum(exponent, axis=-1, keepdims=True)).astype(jnp.bfloat16)
    head_out = jnp.einsum(
        "bmhqk,bkmhd->bqmhd", attention, value_rows, preferred_element_type=jnp.float32
    ).astype(jnp.bfloat16).reshape(tokens, n_mp, width)
    residual_two = residual
    for m in range(n_mp):
        residual_two = residual_two + grouped(dot_t(head_out[:, m], full[0, m, :, 3 * width :]))
    normed_second = layer_norm(residual_two, gain_second).astype(jnp.bfloat16)
    total = residual_two
    for m in range(n_mp):
        hidden = jax.nn.gelu(dot(normed_second, full[1, m]), approximate=False).astype(jnp.bfloat16)
        total = total + grouped(dot_t(hidden, full[2, m]))
    pooled = jnp.sum(total.reshape(own_images, patch_count, features), axis=1) / patch_count
    pooled_norm = layer_norm(pooled, gain_final).astype(jnp.bfloat16)
    image_units = unit_rows(dot(pooled_norm, project_weight)).astype(jnp.bfloat16)

    place = lax.axis_index(("dp", "mp"))
    texts = text_bank.shape[0]
    all_units = lax.all_gather(image_units, ("dp", "mp"), axis=0, tiled=True)
    logits = dot_t(all_units, text_bank)
    highest = jnp.max(logits, axis=1)
    totals = jnp.sum(jnp.exp(logits - highest[:, None]), axis=1)
    text_ids = lax.broadcasted_iota(jnp.int32, logits.shape, 1) + place * texts
    matched = jnp.sum(jnp.where(text_ids == captions[:, None], logits, 0.0), axis=1)
    stats = jnp.stack([highest, totals, matched])
    everyone = lax.all_gather(stats, ("dp", "mp"), axis=0)
    mine = lax.dynamic_slice_in_dim(everyone, place * own_images, own_images, axis=2)
    top = jnp.max(mine[:, 0], axis=0)
    total_exp = jnp.sum(mine[:, 1] * jnp.exp(mine[:, 0] - top[None]), axis=0)
    return top + jnp.log(total_exp) - jnp.sum(mine[:, 2], axis=0) - reference_loss


def solution(mesh):
    placed = (
        P(("dp", "mp"), None, None),
        P(),
        P("dp", None, "mp"),
        P("mp"),
        P("mp", "dp"),
        P(),
        P("dp", "mp"),
        P("mp", "dp"),
        P(),
        P(),
        P(("dp", "mp"), None),
        P(),
        P(("dp", "mp")),
    )
    return jax.shard_map(
        shards, mesh=mesh, in_specs=placed, out_specs=P(("dp", "mp")), check_vma=False
    )
```

```python
import functools

import jax
import jax.numpy as jnp
from jax import lax
from jax.experimental import pallas as pl
from jax.experimental.pallas import tpu as pltpu
from jax.sharding import PartitionSpec as P

MESH = pl.DeviceIdType.MESH
Z, X, Y, D0, D1, S_COL, S_X, S_Y, S_D0, S_D1 = range(10)
KINDS = 10


def flip(index, bit):
    return index + bit - 2 * bit * ((index // bit) % 2)


def gather_kernel(
    n_mp, own_ref, scale_ref, full_ref, scales_ref, send_sem, recv_sem, local_sem, scale_send, scale_recv
):
    parts, rows, _ = own_ref.shape
    dp, mp = lax.axis_index("dp"), lax.axis_index("mp")
    sib, xn, yn = flip(dp, 1), flip(dp, 2), flip(dp, 4)
    dn = flip(xn, 4)
    right, left = lax.rem(mp + 1, n_mp), lax.rem(mp + n_mp - 1, n_mp)

    barrier = pltpu.get_barrier_semaphore()
    for target in ((dp, right), (dp, left), (xn, mp), (yn, mp), (sib, mp)):
        pl.semaphore_signal(barrier, inc=1, device_id=target, device_id_type=MESH)
    pl.semaphore_wait(barrier, 5)

    half = rows // 2

    def slot(part, step, owner, piece):
        source = lax.rem(mp - step + n_mp, n_mp)
        first = owner * rows + (half if piece == 1 else 0)
        count = rows if piece is None else half
        return full_ref.at[part, source, pl.ds(pl.multiple_of(first, half), count), :]

    def copy(kind, part, step, owner, piece, target):
        index = (part * n_mp + step) * KINDS + kind
        place = slot(part, step, owner, piece)
        src = own_ref.at[part] if step == 0 and owner is dp else place
        return pltpu.make_async_remote_copy(
            src_ref=src, dst_ref=place, send_sem=send_sem.at[index], recv_sem=recv_sem.at[index],
            device_id=target, device_id_type=MESH,
        )

    def arrival(kind, part, step, sem_step, owner, piece):
        index = (part * n_mp + sem_step) * KINDS + kind
        place = slot(part, step, owner, piece)
        pltpu.make_async_remote_copy(
            src_ref=place, dst_ref=place, send_sem=send_sem.at[index], recv_sem=recv_sem.at[index],
            device_id=(sib, mp), device_id_type=MESH,
        ).wait_recv()

    def scale_copy(step, source):
        return pltpu.make_async_remote_copy(
            src_ref=scale_ref if step == 0 else scales_ref.at[source], dst_ref=scales_ref.at[source],
            send_sem=scale_send.at[step], recv_sem=scale_recv.at[step],
            device_id=(dp, right), device_id_type=MESH,
        )

    def scale_step(step):
        if step > 0:
            scale_copy(step - 1, lax.rem(mp - step + n_mp, n_mp)).wait_recv()
        if step < n_mp - 1:
            item = scale_copy(step, lax.rem(mp - step + n_mp, n_mp))
            item.start()
            sent.append(item)

    sent = []

    def send(*args):
        item = copy(*args)
        item.start()
        sent.append(item)

    steps = [(part, step) for part in range(parts) for step in range(n_mp)]
    local = []
    for part in range(parts):
        item = pltpu.make_async_copy(own_ref.at[part], slot(part, 0, dp, None), local_sem.at[part])
        item.start()
        local.append(item)
    item = pltpu.make_async_copy(scale_ref, scales_ref.at[mp], local_sem.at[parts])
    item.start()
    local.append(item)

    def along_ring(at):
        if at < len(steps):
            part, step = steps[at]
            if part == 0:
                scale_step(step)
            if step > 0:
                arrival(Z, part, step, step - 1, dp, None)
            if step < n_mp - 1:
                send(Z, part, step, dp, None, (dp, right))

    along_ring(0)
    for at in range(len(steps) + 2):
        along_ring(at + 1)
        if at < len(steps):
            part, step = steps[at]
            send(X, part, step, dp, None, (xn, mp))
            send(Y, part, step, dp, None, (yn, mp))
            send(S_COL, part, step, dp, None, (sib, mp))
        if 0 <= at - 1 < len(steps):
            part, step = steps[at - 1]
            arrival(X, part, step, step, xn, None)
            send(D0, part, step, xn, 0, (yn, mp))
            send(S_X, part, step, xn, None, (sib, mp))
            arrival(Y, part, step, step, yn, None)
            send(D1, part, step, yn, 1, (xn, mp))
            send(S_Y, part, step, yn, None, (sib, mp))
        if 0 <= at - 2 < len(steps):
            part, step = steps[at - 2]
            arrival(D0, part, step, step, dn, 0)
            send(S_D0, part, step, dn, 0, (sib, mp))
            arrival(D1, part, step, step, dn, 1)
            send(S_D1, part, step, dn, 1, (sib, mp))
    for part, step in steps:
        arrival(S_COL, part, step, step, flip(dp, 1), None)
        arrival(S_X, part, step, step, flip(xn, 1), None)
        arrival(S_Y, part, step, step, flip(yn, 1), None)
        arrival(S_D0, part, step, step, flip(dn, 1), 0)
        arrival(S_D1, part, step, step, flip(dn, 1), 1)
    for item in sent:
        item.wait_send()
    for item in local:
        item.wait()


def gather_weights(own, scale, n_dp, n_mp):
    parts, rows, columns = own.shape
    if n_dp != 2 ** 3:
        full = lax.all_gather(own, "dp", axis=1, tiled=True)
        return lax.all_gather(full, "mp", axis=1), lax.all_gather(scale, "mp", axis=0)
    count = parts * n_mp * KINDS
    return pl.pallas_call(
        functools.partial(gather_kernel, n_mp),
        out_shape=(
            jax.ShapeDtypeStruct((parts, n_mp, n_dp * rows, columns), own.dtype),
            jax.ShapeDtypeStruct((n_mp, *scale.shape), scale.dtype),
        ),
        in_specs=[pl.BlockSpec(memory_space=pltpu.VMEM)] * 2,
        out_specs=(pl.BlockSpec(memory_space=pl.ANY), pl.BlockSpec(memory_space=pltpu.VMEM)),
        scratch_shapes=[
            pltpu.SemaphoreType.DMA((count,)),
            pltpu.SemaphoreType.DMA((count,)),
            pltpu.SemaphoreType.DMA((parts + 1,)),
            pltpu.SemaphoreType.DMA((n_mp,)),
            pltpu.SemaphoreType.DMA((n_mp,)),
        ],
        compiler_params=pltpu.CompilerParams(collective_id=0, has_side_effects=True),
        name="gather_weights",
    )(own, scale)


def exchange_kernel(n_dp, n_mp, spread, own_ref, all_ref, send_sem, recv_sem, local_sem):
    dp, mp = lax.axis_index("dp"), lax.axis_index("mp")
    count = n_dp * n_mp
    me = dp * n_mp + mp
    barrier = pltpu.get_barrier_semaphore()

    def peer(shift):
        other = lax.rem(me + shift, count)
        return other, (other // n_mp, lax.rem(other, n_mp))

    def greet(shift, carry):
        pl.semaphore_signal(barrier, inc=1, device_id=peer(shift)[1], device_id_type=MESH)
        return carry

    lax.fori_loop(1, count, greet, 0)
    pl.semaphore_wait(barrier, count - 1)
    local = pltpu.make_async_copy(own_ref.at[me] if spread else own_ref, all_ref.at[me], local_sem)
    local.start()

    def copy(shift):
        other, target = peer(shift)
        return pltpu.make_async_remote_copy(
            src_ref=own_ref.at[other] if spread else own_ref, dst_ref=all_ref.at[me],
            send_sem=send_sem.at[shift], recv_sem=recv_sem.at[shift],
            device_id=target, device_id_type=MESH,
        )

    def begin(shift, carry):
        copy(shift).start()
        return carry

    def finish(shift, carry):
        source = lax.rem(me - shift + count, count)
        pltpu.make_async_remote_copy(
            src_ref=all_ref.at[source], dst_ref=all_ref.at[source],
            send_sem=send_sem.at[shift], recv_sem=recv_sem.at[shift],
            device_id=peer(shift)[1], device_id_type=MESH,
        ).wait_recv()
        copy(shift).wait_send()
        return carry

    lax.fori_loop(1, count, begin, 0)
    lax.fori_loop(1, count, finish, 0)
    local.wait()


def exchange(own, n_dp, n_mp, spread, collective_id):
    count = n_dp * n_mp
    block = own.shape[1:] if spread else own.shape
    return pl.pallas_call(
        functools.partial(exchange_kernel, n_dp, n_mp, spread),
        out_shape=jax.ShapeDtypeStruct((count, *block), own.dtype),
        in_specs=[pl.BlockSpec(memory_space=pltpu.VMEM)],
        out_specs=pl.BlockSpec(memory_space=pltpu.VMEM),
        scratch_shapes=[
            pltpu.SemaphoreType.DMA((count,)),
            pltpu.SemaphoreType.DMA((count,)),
            pltpu.SemaphoreType.DMA,
        ],
        compiler_params=pltpu.CompilerParams(collective_id=collective_id, has_side_effects=True),
        name="spread_stats" if spread else "share_units",
    )(own)


def feed_kernel(normed_ref, up_ref, down_ref, residual_ref, total_ref):
    @pl.when(pl.program_id(0) == 0)
    def _():
        total_ref[...] = residual_ref[...]

    upper = dot(normed_ref[...], up_ref[...])
    hidden = (0.5 * upper * (1.0 + lax.erf(upper * 0.5 ** 0.5))).astype(jnp.bfloat16)
    total_ref[...] += grouped(dot_t(hidden, down_ref[...]))


def feed_forward(normed, full, residual):
    _, groups, features, width = full.shape
    weight = lambda part: pl.BlockSpec((None, None, features, width), lambda m: (part, m, 0, 0))
    whole = pl.BlockSpec(normed.shape, lambda m: (0, 0))
    return pl.pallas_call(
        feed_kernel,
        grid=(groups,),
        out_shape=jax.ShapeDtypeStruct(residual.shape, jnp.float32),
        in_specs=[whole, weight(1), weight(2), whole],
        out_specs=whole,
        compiler_params=pltpu.CompilerParams(dimension_semantics=("arbitrary",)),
        name="feed_forward",
    )(normed, full, full, residual)


def layer_norm(values, gain):
    centre = values - jnp.mean(values, axis=-1, keepdims=True)
    spread = jnp.mean(centre * centre, axis=-1, keepdims=True)
    return centre * lax.rsqrt(spread + 1e-06) * gain


def unit_rows(values):
    return values * lax.rsqrt(jnp.sum(values * values, axis=-1, keepdims=True) + 1e-06)


def dot(left, right):
    return jnp.dot(left, right, preferred_element_type=jnp.float32)


def dot_t(left, right):
    return lax.dot_general(left, right, (((1,), (1,)), ((), ())), preferred_element_type=jnp.float32)


def grouped(values):
    return values.astype(jnp.bfloat16).astype(jnp.float32)


def shards(
    patches,
    gain_first,
    joint_weight,
    head_scale,
    output_weight,
    gain_second,
    up_weight,
    down_weight,
    gain_final,
    project_weight,
    text_bank,
    captions,
    reference_loss,
):
    n_dp, n_mp = lax.axis_size("dp"), lax.axis_size("mp")
    own_images, patch_count, features = patches.shape
    rows = joint_weight.shape[0]
    local_heads = head_scale.shape[0]
    width = joint_weight.shape[2]
    head_width = width // local_heads
    tokens = own_images * patch_count

    attention_part = jnp.concatenate([joint_weight.reshape(rows, 3 * width), output_weight.T], axis=1)
    own = jnp.stack([attention_part, up_weight, down_weight.T])
    full, scales = gather_weights(own, head_scale[None, :], n_dp, n_mp)

    residual = patches.astype(jnp.float32).reshape(tokens, features)
    normed_first = layer_norm(residual, gain_first).astype(jnp.bfloat16)
    residual_two = residual
    for m in range(n_mp):
        joint = dot(normed_first, full[0, m])[:, : 3 * width]
        joint = joint.reshape(own_images, patch_count, 3, local_heads, head_width)
        queries = unit_rows(joint[:, :, 0]).astype(jnp.bfloat16)
        key_rows = unit_rows(joint[:, :, 1]).astype(jnp.bfloat16)
        value_rows = joint[:, :, 2].astype(jnp.bfloat16)
        scores = jnp.einsum("bqhd,bkhd->bhqk", queries, key_rows, preferred_element_type=jnp.float32)
        exponent = jnp.exp(scores * scales[m, 0][None, :, None, None])
        attention = (exponent / jnp.sum(exponent, axis=-1, keepdims=True)).astype(jnp.bfloat16)
        head_out = jnp.einsum(
            "bhqk,bkhd->bqhd", attention, value_rows, preferred_element_type=jnp.float32
        ).astype(jnp.bfloat16).reshape(tokens, width)
        residual_two = residual_two + grouped(dot_t(head_out, full[0, m, :, 3 * width :]))
    normed_second = layer_norm(residual_two, gain_second).astype(jnp.bfloat16)
    total = feed_forward(normed_second, full, residual_two)
    pooled = jnp.sum(total.reshape(own_images, patch_count, features), axis=1) / patch_count
    pooled_norm = layer_norm(pooled, gain_final).astype(jnp.bfloat16)
    image_units = unit_rows(dot(pooled_norm, project_weight)).astype(jnp.bfloat16)

    place = lax.axis_index(("dp", "mp"))
    texts = text_bank.shape[0]
    all_units = exchange(image_units, n_dp, n_mp, False, 1).reshape(-1, image_units.shape[1])
    logits = dot_t(all_units, text_bank)
    highest = jnp.max(logits, axis=1)
    totals = jnp.sum(jnp.exp(logits - highest[:, None]), axis=1)
    text_ids = lax.broadcasted_iota(jnp.int32, logits.shape, 1) + place * texts
    matched = jnp.sum(jnp.where(text_ids == captions[:, None], logits, 0.0), axis=1)
    stats = jnp.stack([highest, totals, matched]).reshape(3, n_dp * n_mp, own_images)
    mine = exchange(stats.transpose(1, 0, 2), n_dp, n_mp, True, 2)
    top = jnp.max(mine[:, 0], axis=0)
    total_exp = jnp.sum(mine[:, 1] * jnp.exp(mine[:, 0] - top[None]), axis=0)
    return top + jnp.log(total_exp) - jnp.sum(mine[:, 2], axis=0) - reference_loss


def solution(mesh):
    placed = (
        P(("dp", "mp"), None, None),
        P(),
        P("dp", None, "mp"),
        P("mp"),
        P("mp", "dp"),
        P(),
        P("dp", "mp"),
        P("mp", "dp"),
        P(),
        P(),
        P(("dp", "mp"), None),
        P(),
        P(("dp", "mp")),
    )
    return jax.shard_map(
        shards, mesh=mesh, in_specs=placed, out_specs=P(("dp", "mp")), check_vma=False
    )
```

```python
import functools

import jax
import jax.numpy as jnp
from jax import lax
from jax.experimental import pallas as pl
from jax.experimental.pallas import tpu as pltpu
from jax.sharding import PartitionSpec as P

MESH = pl.DeviceIdType.MESH
Z, X, Y, D0, D1, S_COL, S_X, S_Y, S_D0, S_D1 = range(10)
KINDS = 10


def flip(index, bit):
    return index + bit - 2 * bit * ((index // bit) % 2)


def gather_kernel(
    n_mp, own_ref, scale_ref, full_ref, scales_ref, send_sem, recv_sem, local_sem, scale_send, scale_recv
):
    parts, rows, _ = own_ref.shape
    dp, mp = lax.axis_index("dp"), lax.axis_index("mp")
    sib, xn, yn = flip(dp, 1), flip(dp, 2), flip(dp, 4)
    dn = flip(xn, 4)
    right, left = lax.rem(mp + 1, n_mp), lax.rem(mp + n_mp - 1, n_mp)

    barrier = pltpu.get_barrier_semaphore()
    for target in ((dp, right), (dp, left), (xn, mp), (yn, mp), (sib, mp)):
        pl.semaphore_signal(barrier, inc=1, device_id=target, device_id_type=MESH)
    pl.semaphore_wait(barrier, 5)

    half = rows // 2

    def slot(part, step, owner, piece):
        source = lax.rem(mp - step + n_mp, n_mp)
        first = owner * rows + (half if piece == 1 else 0)
        count = rows if piece is None else half
        return full_ref.at[part, source, pl.ds(pl.multiple_of(first, half), count), :]

    def copy(kind, part, step, owner, piece, target):
        index = (part * n_mp + step) * KINDS + kind
        place = slot(part, step, owner, piece)
        src = own_ref.at[part] if step == 0 and owner is dp else place
        return pltpu.make_async_remote_copy(
            src_ref=src, dst_ref=place, send_sem=send_sem.at[index], recv_sem=recv_sem.at[index],
            device_id=target, device_id_type=MESH,
        )

    def arrival(kind, part, step, sem_step, owner, piece):
        index = (part * n_mp + sem_step) * KINDS + kind
        place = slot(part, step, owner, piece)
        pltpu.make_async_remote_copy(
            src_ref=place, dst_ref=place, send_sem=send_sem.at[index], recv_sem=recv_sem.at[index],
            device_id=(sib, mp), device_id_type=MESH,
        ).wait_recv()

    def scale_copy(step, source):
        return pltpu.make_async_remote_copy(
            src_ref=scale_ref if step == 0 else scales_ref.at[source], dst_ref=scales_ref.at[source],
            send_sem=scale_send.at[step], recv_sem=scale_recv.at[step],
            device_id=(dp, right), device_id_type=MESH,
        )

    def scale_step(step):
        if step > 0:
            scale_copy(step - 1, lax.rem(mp - step + n_mp, n_mp)).wait_recv()
        if step < n_mp - 1:
            item = scale_copy(step, lax.rem(mp - step + n_mp, n_mp))
            item.start()
            sent.append(item)

    sent = []

    def send(*args):
        item = copy(*args)
        item.start()
        sent.append(item)

    steps = [(part, step) for part in range(parts) for step in range(n_mp)]
    local = []
    for part in range(parts):
        item = pltpu.make_async_copy(own_ref.at[part], slot(part, 0, dp, None), local_sem.at[part])
        item.start()
        local.append(item)
    item = pltpu.make_async_copy(scale_ref, scales_ref.at[mp], local_sem.at[parts])
    item.start()
    local.append(item)

    def along_ring(at):
        if at < len(steps):
            part, step = steps[at]
            if part == 0:
                scale_step(step)
            if step > 0:
                arrival(Z, part, step, step - 1, dp, None)
            if step < n_mp - 1:
                send(Z, part, step, dp, None, (dp, right))

    along_ring(0)
    for at in range(len(steps) + 2):
        along_ring(at + 1)
        if at < len(steps):
            part, step = steps[at]
            send(X, part, step, dp, None, (xn, mp))
            send(Y, part, step, dp, None, (yn, mp))
            send(S_COL, part, step, dp, None, (sib, mp))
        if 0 <= at - 1 < len(steps):
            part, step = steps[at - 1]
            arrival(X, part, step, step, xn, None)
            send(D0, part, step, xn, 0, (yn, mp))
            send(S_X, part, step, xn, None, (sib, mp))
            arrival(Y, part, step, step, yn, None)
            send(D1, part, step, yn, 1, (xn, mp))
            send(S_Y, part, step, yn, None, (sib, mp))
        if 0 <= at - 2 < len(steps):
            part, step = steps[at - 2]
            arrival(D0, part, step, step, dn, 0)
            send(S_D0, part, step, dn, 0, (sib, mp))
            arrival(D1, part, step, step, dn, 1)
            send(S_D1, part, step, dn, 1, (sib, mp))
    for part, step in steps:
        arrival(S_COL, part, step, step, flip(dp, 1), None)
        arrival(S_X, part, step, step, flip(xn, 1), None)
        arrival(S_Y, part, step, step, flip(yn, 1), None)
        arrival(S_D0, part, step, step, flip(dn, 1), 0)
        arrival(S_D1, part, step, step, flip(dn, 1), 1)
    for item in sent:
        item.wait_send()
    for item in local:
        item.wait()


def gather_weights(own, scale, n_dp, n_mp):
    parts, rows, columns = own.shape
    if n_dp != 2 ** 3:
        full = lax.all_gather(own, "dp", axis=1, tiled=True)
        return lax.all_gather(full, "mp", axis=1), lax.all_gather(scale, "mp", axis=0)
    count = parts * n_mp * KINDS
    return pl.pallas_call(
        functools.partial(gather_kernel, n_mp),
        out_shape=(
            jax.ShapeDtypeStruct((parts, n_mp, n_dp * rows, columns), own.dtype),
            jax.ShapeDtypeStruct((n_mp, *scale.shape), scale.dtype),
        ),
        in_specs=[pl.BlockSpec(memory_space=pltpu.VMEM)] * 2,
        out_specs=(pl.BlockSpec(memory_space=pl.ANY), pl.BlockSpec(memory_space=pltpu.VMEM)),
        scratch_shapes=[
            pltpu.SemaphoreType.DMA((count,)),
            pltpu.SemaphoreType.DMA((count,)),
            pltpu.SemaphoreType.DMA((parts + 1,)),
            pltpu.SemaphoreType.DMA((n_mp,)),
            pltpu.SemaphoreType.DMA((n_mp,)),
        ],
        compiler_params=pltpu.CompilerParams(collective_id=0, has_side_effects=True),
        name="gather_weights",
    )(own, scale)


def exchange_kernel(n_dp, n_mp, spread, own_ref, all_ref, send_sem, recv_sem, local_sem):
    dp, mp = lax.axis_index("dp"), lax.axis_index("mp")
    count = n_dp * n_mp
    me = dp * n_mp + mp
    barrier = pltpu.get_barrier_semaphore()

    def peer(shift):
        other = lax.rem(me + shift, count)
        return other, (other // n_mp, lax.rem(other, n_mp))

    def greet(shift, carry):
        pl.semaphore_signal(barrier, inc=1, device_id=peer(shift)[1], device_id_type=MESH)
        return carry

    lax.fori_loop(1, count, greet, 0)
    pl.semaphore_wait(barrier, count - 1)
    local = pltpu.make_async_copy(own_ref.at[me] if spread else own_ref, all_ref.at[me], local_sem)
    local.start()

    def copy(shift):
        other, target = peer(shift)
        return pltpu.make_async_remote_copy(
            src_ref=own_ref.at[other] if spread else own_ref, dst_ref=all_ref.at[me],
            send_sem=send_sem.at[shift], recv_sem=recv_sem.at[shift],
            device_id=target, device_id_type=MESH,
        )

    def begin(shift, carry):
        copy(shift).start()
        return carry

    def finish(shift, carry):
        source = lax.rem(me - shift + count, count)
        pltpu.make_async_remote_copy(
            src_ref=all_ref.at[source], dst_ref=all_ref.at[source],
            send_sem=send_sem.at[shift], recv_sem=recv_sem.at[shift],
            device_id=peer(shift)[1], device_id_type=MESH,
        ).wait_recv()
        copy(shift).wait_send()
        return carry

    lax.fori_loop(1, count, begin, 0)
    lax.fori_loop(1, count, finish, 0)
    local.wait()


def exchange(own, n_dp, n_mp, spread, collective_id):
    count = n_dp * n_mp
    block = own.shape[1:] if spread else own.shape
    return pl.pallas_call(
        functools.partial(exchange_kernel, n_dp, n_mp, spread),
        out_shape=jax.ShapeDtypeStruct((count, *block), own.dtype),
        in_specs=[pl.BlockSpec(memory_space=pltpu.VMEM)],
        out_specs=pl.BlockSpec(memory_space=pltpu.VMEM),
        scratch_shapes=[
            pltpu.SemaphoreType.DMA((count,)),
            pltpu.SemaphoreType.DMA((count,)),
            pltpu.SemaphoreType.DMA,
        ],
        compiler_params=pltpu.CompilerParams(collective_id=collective_id, has_side_effects=True),
        name="spread_stats" if spread else "share_units",
    )(own)


def attention_kernel(images, heads, scale_ref, normed_ref, weight_ref, residual_ref, total_ref, head_ref):
    group = pl.program_id(0)

    @pl.when(group == 0)
    def _():
        total_ref[...] = residual_ref[...]

    tokens, width = head_ref.shape
    head_width = width // heads
    joint = dot(normed_ref[...], weight_ref[:, : 3 * width])

    def rows_of(part, head):
        first = part * width + head * head_width
        return joint[:, first : first + head_width]

    def by_image(values):
        return values.astype(jnp.bfloat16).reshape(images, tokens // images, head_width)

    for head in range(heads):
        queries = by_image(unit_rows(rows_of(0, head)))
        key_rows = by_image(unit_rows(rows_of(1, head)))
        value_rows = by_image(rows_of(2, head))
        scores = jnp.einsum("bqd,bkd->bqk", queries, key_rows, preferred_element_type=jnp.float32)
        exponent = jnp.exp(scores * scale_ref[group, head])
        attention = (exponent / jnp.sum(exponent, axis=-1, keepdims=True)).astype(jnp.bfloat16)
        mixed = jnp.einsum("bqk,bkd->bqd", attention, value_rows, preferred_element_type=jnp.float32)
        head_ref[:, head * head_width : (head + 1) * head_width] = mixed.astype(jnp.bfloat16).reshape(
            tokens, head_width
        )
    total_ref[...] += grouped(dot_t(head_ref[...], weight_ref[:, 3 * width :]))


def attend(scales, normed, full, residual, images, width):
    _, groups, features, columns = full.shape
    whole = pl.BlockSpec(normed.shape, lambda m: (0, 0))
    return pl.pallas_call(
        functools.partial(attention_kernel, images, scales.shape[1]),
        grid=(groups,),
        out_shape=jax.ShapeDtypeStruct(residual.shape, jnp.float32),
        in_specs=[
            pl.BlockSpec(memory_space=pltpu.SMEM),
            whole,
            pl.BlockSpec((None, None, features, columns), lambda m: (0, m, 0, 0)),
            whole,
        ],
        out_specs=whole,
        scratch_shapes=[pltpu.VMEM((normed.shape[0], width), jnp.bfloat16)],
        compiler_params=pltpu.CompilerParams(dimension_semantics=("arbitrary",)),
        name="attend",
    )(scales, normed, full, residual)


def feed_kernel(normed_ref, up_ref, down_ref, residual_ref, total_ref):
    @pl.when(pl.program_id(0) == 0)
    def _():
        total_ref[...] = residual_ref[...]

    upper = dot(normed_ref[...], up_ref[...])
    hidden = (0.5 * upper * (1.0 + lax.erf(upper * 0.5 ** 0.5))).astype(jnp.bfloat16)
    total_ref[...] += grouped(dot_t(hidden, down_ref[...]))


def feed_forward(normed, full, residual):
    _, groups, features, width = full.shape
    weight = lambda part: pl.BlockSpec((None, None, features, width), lambda m: (part, m, 0, 0))
    whole = pl.BlockSpec(normed.shape, lambda m: (0, 0))
    return pl.pallas_call(
        feed_kernel,
        grid=(groups,),
        out_shape=jax.ShapeDtypeStruct(residual.shape, jnp.float32),
        in_specs=[whole, weight(1), weight(2), whole],
        out_specs=whole,
        compiler_params=pltpu.CompilerParams(dimension_semantics=("arbitrary",)),
        name="feed_forward",
    )(normed, full, full, residual)


def layer_norm(values, gain):
    centre = values - jnp.mean(values, axis=-1, keepdims=True)
    spread = jnp.mean(centre * centre, axis=-1, keepdims=True)
    return centre * lax.rsqrt(spread + 1e-06) * gain


def unit_rows(values):
    return values * lax.rsqrt(jnp.sum(values * values, axis=-1, keepdims=True) + 1e-06)


def dot(left, right):
    return jnp.dot(left, right, preferred_element_type=jnp.float32)


def dot_t(left, right):
    return lax.dot_general(left, right, (((1,), (1,)), ((), ())), preferred_element_type=jnp.float32)


def grouped(values):
    return values.astype(jnp.bfloat16).astype(jnp.float32)


def shards(
    patches,
    gain_first,
    joint_weight,
    head_scale,
    output_weight,
    gain_second,
    up_weight,
    down_weight,
    gain_final,
    project_weight,
    text_bank,
    captions,
    reference_loss,
):
    n_dp, n_mp = lax.axis_size("dp"), lax.axis_size("mp")
    own_images, patch_count, features = patches.shape
    rows = joint_weight.shape[0]
    width = joint_weight.shape[2]
    tokens = own_images * patch_count

    attention_part = jnp.concatenate([joint_weight.reshape(rows, 3 * width), output_weight.T], axis=1)
    own = jnp.stack([attention_part, up_weight, down_weight.T])
    full, scales = gather_weights(own, head_scale[None, :], n_dp, n_mp)

    residual = patches.astype(jnp.float32).reshape(tokens, features)
    normed_first = layer_norm(residual, gain_first).astype(jnp.bfloat16)
    residual_two = attend(scales[:, 0], normed_first, full, residual, own_images, width)
    normed_second = layer_norm(residual_two, gain_second).astype(jnp.bfloat16)
    total = feed_forward(normed_second, full, residual_two)
    pooled = jnp.sum(total.reshape(own_images, patch_count, features), axis=1) / patch_count
    pooled_norm = layer_norm(pooled, gain_final).astype(jnp.bfloat16)
    image_units = unit_rows(dot(pooled_norm, project_weight)).astype(jnp.bfloat16)

    place = lax.axis_index(("dp", "mp"))
    texts = text_bank.shape[0]
    all_units = exchange(image_units, n_dp, n_mp, False, 1).reshape(-1, image_units.shape[1])
    logits = dot_t(all_units, text_bank)
    highest = jnp.max(logits, axis=1)
    totals = jnp.sum(jnp.exp(logits - highest[:, None]), axis=1)
    text_ids = lax.broadcasted_iota(jnp.int32, logits.shape, 1) + place * texts
    matched = jnp.sum(jnp.where(text_ids == captions[:, None], logits, 0.0), axis=1)
    stats = jnp.stack([highest, totals, matched]).reshape(3, n_dp * n_mp, own_images)
    mine = exchange(stats.transpose(1, 0, 2), n_dp, n_mp, True, 2)
    top = jnp.max(mine[:, 0], axis=0)
    total_exp = jnp.sum(mine[:, 1] * jnp.exp(mine[:, 0] - top[None]), axis=0)
    return top + jnp.log(total_exp) - jnp.sum(mine[:, 2], axis=0) - reference_loss


def solution(mesh):
    placed = (
        P(("dp", "mp"), None, None),
        P(),
        P("dp", None, "mp"),
        P("mp"),
        P("mp", "dp"),
        P(),
        P("dp", "mp"),
        P("mp", "dp"),
        P(),
        P(),
        P(("dp", "mp"), None),
        P(),
        P(("dp", "mp")),
    )
    return jax.shard_map(
        shards, mesh=mesh, in_specs=placed, out_specs=P(("dp", "mp")), check_vma=False
    )
```
